512 devices in a mesh: frame: 32 (over x, z_lo), view: 16 (over y, z_hi, core).
Axes of the slice: x: 4, y: 4, z: 16 (z_hi: 2, z_lo: 8; z = z_hi * 8 + z_lo), core: 2. Of those that a mesh axis runs over, the one named last changes fastest.
Arguments:
- t_query: bfloat16 [16, 64, 64, 1024], P('view', 'frame'), may hold values from -8 to 8
- t_key: bfloat16 [16, 64, 64, 1024], P('view', 'frame'), may hold values from -8 to 8
- t_value: bfloat16 [16, 64, 64, 1024], P('view', 'frame'), may hold values from -6 to 6
- t_grad: bfloat16 [16, 64, 64, 1024], P('view', 'frame'), may hold values from -6 to 6
- v_query: bfloat16 [16, 64, 64, 1024], P('view', 'frame'), may hold values from -8 to 8
- v_key: bfloat16 [16, 64, 64, 1024], P('view', 'frame'), may hold values from -8 to 8
- v_value: bfloat16 [16, 64, 64, 1024], P('view', 'frame'), may hold values from -6 to 6
- v_grad: bfloat16 [16, 64, 64, 1024], P('view', 'frame'), may hold values from -6 to 6
Outputs:
- t_query_grad: bfloat16 [16, 64, 64, 1024], P('view', 'frame')
- t_key_grad: bfloat16 [16, 64, 64, 1024], P('view', 'frame')
- t_value_grad: bfloat16 [16, 64, 64, 1024], P('view', 'frame')
- v_query_grad: bfloat16 [16, 64, 64, 1024], P('view', 'frame')
- v_key_grad: bfloat16 [16, 64, 64, 1024], P('view', 'frame')
- v_value_grad: bfloat16 [16, 64, 64, 1024], P('view', 'frame')
The draws below stay inside these ranges and needn't reach their ends.
All inputs are finite; a program needn't handle non-finite values.
Results may differ from the reference program's by a relative error of at most 0.0085.
Values may be sent and summed in bfloat16 or wider, within the bound.
A program may use at most 64 MiB of HBM per device.

```python
import jax
import jax.numpy as jnp
from jax import lax

HEADS = 16
HEAD_DIM = 64
ROWS = 8
COLS = 8
WIDTH = 1024
VIEWS = 16
FRAMES = 64
PATCHES = 64


def draw_pair(key, block_tag):
    shape = (VIEWS, FRAMES, PATCHES, HEADS * HEAD_DIM)
    query_all = jnp.clip(jax.random.normal(jax.random.fold_in(key, block_tag + 1), shape, jnp.float32), -6.0, 6.0)
    key_all = jnp.clip(jax.random.normal(jax.random.fold_in(key, block_tag + 2), shape, jnp.float32), -6.0, 6.0)
    return (query_all.astype(jnp.bfloat16), key_all.astype(jnp.bfloat16))


def draw_t_query(key, part):
    return draw_pair(key, 100)[0]


def draw_t_key(key, part):
    return draw_pair(key, 100)[1]


def draw_v_query(key, part):
    return draw_pair(key, 200)[0]


def draw_v_key(key, part):
    return draw_pair(key, 200)[1]


def level_of(key, dims, cuts, smallest, largest):
    loudness = 1.0
    for dim, blocks in cuts:
        steps = jax.random.uniform(jax.random.fold_in(jax.random.fold_in(key, 6), dim), (blocks,), jnp.float32, smallest / len(cuts), largest / len(cuts))
        loudness = loudness * jnp.repeat(jnp.exp(steps), dims[dim] // blocks).reshape((-1,) + (1,) * (len(dims) - 1 - dim))
    return loudness


def gaussian(own_key, dims, deviation, most, cuts=(), dtype=jnp.bfloat16):
    values = jax.random.normal(own_key, dims, jnp.float32) * deviation
    if len(cuts) > 0:
        values = level_of(own_key, dims, cuts, -0.22, 0.18) * values
    return jnp.clip(values, min=-most, max=most).astype(dtype)


def setup_inputs(seed: int = 0) -> dict:
    arg_keys = jax.random.split(jax.random.key(seed), 9)
    return {
        "t_query": draw_t_query(jax.random.fold_in(arg_keys[8], 71), 0),
        "t_key": draw_t_key(jax.random.fold_in(arg_keys[8], 71), 0),
        "t_value": gaussian(arg_keys[2], (VIEWS, FRAMES, PATCHES, WIDTH), 1.0, 6.0, ((0, 16), (1, 32))),
        "t_grad": gaussian(arg_keys[3], (VIEWS, FRAMES, PATCHES, WIDTH), 1.0, 6.0, ((0, 16), (1, 32))),
        "v_query": draw_v_query(jax.random.fold_in(arg_keys[8], 71), 0),
        "v_key": draw_v_key(jax.random.fold_in(arg_keys[8], 71), 0),
        "v_value": gaussian(arg_keys[6], (VIEWS, FRAMES, PATCHES, WIDTH), 1.0, 6.0, ((0, 16), (1, 32))),
        "v_grad": gaussian(arg_keys[7], (VIEWS, FRAMES, PATCHES, WIDTH), 1.0, 6.0, ((0, 16), (1, 32))),
    }


def widen(array):
    return array.astype(jnp.float32)


def attention_backward(query_block, key_block, value_block, grad_block, query_spec, key_spec, score_spec, key_count):
    scaling = HEAD_DIM ** -0.5
    key_axes = tuple(range(-key_count, 0))
    scores = jnp.einsum(query_spec + "," + key_spec + "->" + score_spec, widen(query_block), widen(key_block)) * scaling
    row_max = jnp.max(scores, axis=key_axes, keepdims=True)
    exponent = jnp.exp(scores - row_max)
    weights = exponent / jnp.sum(exponent, axis=key_axes, keepdims=True)
    rounded = lax.optimization_barrier(weights.astype(jnp.bfloat16))
    value_grad = jnp.einsum(score_spec + "," + query_spec + "->" + key_spec, widen(rounded), widen(grad_block))
    grad_weights = jnp.einsum(query_spec + "," + key_spec + "->" + score_spec, widen(grad_block), widen(value_block))
    row_delta = jnp.sum(weights * grad_weights, axis=key_axes, keepdims=True)
    grad_scores = lax.optimization_barrier((weights * (grad_weights - row_delta)).astype(jnp.bfloat16))
    query_grad = jnp.einsum(score_spec + "," + key_spec + "->" + query_spec, widen(grad_scores), widen(key_block)) * scaling
    key_grad = jnp.einsum(score_spec + "," + query_spec + "->" + key_spec, widen(grad_scores), widen(query_block)) * scaling
    return query_grad.astype(jnp.bfloat16), key_grad.astype(jnp.bfloat16), value_grad.astype(jnp.bfloat16)


def reference(t_query, t_key, t_value, t_grad, v_query, v_key, v_value, v_grad):
    shape_five = (VIEWS, FRAMES, PATCHES, HEADS, HEAD_DIM)
    temporal_in = tuple(array.reshape(shape_five) for array in (t_query, t_key, t_value, t_grad))

    def per_view(pieces):
        return attention_backward(pieces[0], pieces[1], pieces[2], pieces[3], "fphd", "gphd", "phfg", 1)

    temporal_out = lax.map(per_view, temporal_in)
    temporal_out = tuple(array.reshape(VIEWS, FRAMES, PATCHES, WIDTH) for array in temporal_out)

    shape_six = (VIEWS, FRAMES, ROWS, COLS, HEADS, HEAD_DIM)
    view_in = tuple(jnp.moveaxis(array.reshape(shape_six), 1, 0) for array in (v_query, v_key, v_value, v_grad))

    def per_frame(pieces):
        return attention_backward(pieces[0], pieces[1], pieces[2], pieces[3], "vrchd", "wrehd", "rhvcwe", 2)

    view_out = lax.map(per_frame, view_in)
    view_out = tuple(jnp.moveaxis(array, 0, 1).reshape(VIEWS, FRAMES, PATCHES, WIDTH) for array in view_out)
    return (temporal_out[0], temporal_out[1], temporal_out[2], view_out[0], view_out[1], view_out[2])
```

```python
import functools

import jax
import jax.numpy as jnp
from jax import lax
from jax.experimental import pallas as pl
from jax.experimental.pallas import tpu as pltpu
from jax.sharding import PartitionSpec as P

MESH = pl.DeviceIdType.MESH
HEAD_DIM = 64
LANES = 256
HALF = 128
GROUP = LANES // HEAD_DIM
ROW = 8
F32 = jnp.float32
BF16 = jnp.bfloat16


def flip(index, mask, bits):
    total = 0
    for bit in range(bits):
        width = 1 << bit
        one = lax.rem(lax.div(index, width), 2)
        two = lax.rem(lax.div(mask, width), 2)
        total = total + (one + two - 2 * one * two) * width
    return total


def dot(left, right, left_axis, right_axis):
    return lax.dot_general(
        left, right, (((left_axis,), (right_axis,)), ((), ())), preferred_element_type=F32
    )


def masks(rows, dtype):
    lane = lax.broadcasted_iota(jnp.int32, (rows, LANES), 1)
    return [
        jnp.where((lane >= h * HEAD_DIM) & (lane < (h + 1) * HEAD_DIM), 1.0, 0.0).astype(dtype)
        for h in range(GROUP)
    ]


def attention(query, key, value, grad):
    rows = query.shape[0]
    scaling = HEAD_DIM ** (-0.5)
    narrow, wide = masks(rows, BF16), masks(rows, F32)
    queries = jnp.concatenate([query * m for m in narrow], axis=0)
    grads = jnp.concatenate([grad * m for m in narrow], axis=0)
    scores = dot(key, queries, 1, 1) * scaling
    exponent = jnp.exp(scores - jnp.max(scores, axis=0, keepdims=True))
    weights = exponent / jnp.sum(exponent, axis=0, keepdims=True)
    grad_weights = dot(value, grads, 1, 1)
    delta = jnp.sum(weights * grad_weights, axis=0, keepdims=True)
    grad_scores = (weights * (grad_weights - delta)).astype(BF16)
    value_grad = dot(weights.astype(BF16), grads, 1, 0)
    key_grad = dot(grad_scores, queries, 1, 0) * scaling
    spread = dot(grad_scores, key, 0, 0)
    query_grad = spread[:rows] * wide[0]
    for h in range(1, GROUP):
        query_grad = query_grad + spread[h * rows : (h + 1) * rows] * wide[h]
    return query_grad * scaling, key_grad, value_grad


def kernel(frames, views, *refs):
    t_in, v_in, t_out, v_out = refs[:4], refs[4:8], refs[8:11], refs[11:14]
    t_got, v_got, t_made, v_made, t_wide, o_wide, send, recv = refs[14:]
    frame, view = lax.axis_index("frame"), lax.axis_index("view")
    local = 2
    frame_bits, view_bits = frames.bit_length() - 1, views.bit_length() - 1
    lane_groups = 1024 // LANES

    barrier = pltpu.get_barrier_semaphore()

    def greet_view(k, _):
        pl.semaphore_signal(
            barrier, inc=1, device_id=(frame, flip(view, k, view_bits)), device_id_type=MESH
        )
        return 0

    def greet_frame(k, _):
        pl.semaphore_signal(
            barrier, inc=1, device_id=(flip(frame, k, frame_bits), view), device_id_type=MESH
        )
        return 0

    lax.fori_loop(1, views, greet_view, 0)
    lax.fori_loop(1, frames, greet_frame, 0)
    pl.semaphore_wait(barrier, views + frames - 2)

    def unit(ref, index):
        row = pl.multiple_of(lax.rem(index, 8) * ROW, ROW)
        return ref.at[lax.div(index, 8), pl.ds(row, ROW), :]

    def part(ref, index):
        row = pl.multiple_of(lax.div(index, lane_groups) * ROW, ROW)
        lane = pl.multiple_of(lax.rem(index, lane_groups) * LANES, LANES)
        return ref.at[:, pl.ds(row, ROW), pl.ds(lane, LANES)]

    def own_frames(ref, index):
        return ref.at[pl.ds(index * local, local)]

    def exchange(count, bits, axis, sources, targets, take, put, first):
        me = frame if axis == "frame" else view

        def step(k, _):
            peer = flip(me, k, bits)
            where = (peer, view) if axis == "frame" else (frame, peer)
            for i, (source, target) in enumerate(zip(sources, targets)):
                pltpu.make_async_remote_copy(
                    src_ref=take(source, peer),
                    dst_ref=put(target, me),
                    send_sem=send.at[first + i],
                    recv_sem=recv.at[first + i],
                    device_id=where,
                    device_id_type=MESH,
                ).start()
            return 0

        for i, (source, target) in enumerate(zip(sources, targets)):
            pltpu.make_async_copy(take(source, me), put(target, me), recv.at[first + i]).start()
        lax.fori_loop(1, count, step, 0)

    def landed(targets, first):
        for i, target in enumerate(targets):
            pltpu.make_async_copy(target, target, recv.at[first + i]).wait()

    def left(count, piece, first, number):
        for i in range(number):
            sent = piece.at[pl.ds(0, count)]
            pltpu.make_async_copy(sent, sent, send.at[first + i]).wait()

    t_into = [t_got.at[i] for i in range(4)]
    v_into = [v_got.at[i] for i in range(4)]
    t_from = [t_made.at[i] for i in range(3)]
    v_from = [v_made.at[i] for i in range(3)]

    exchange(views, view_bits, "view", v_in, v_into, unit, lambda r, i: r.at[i], 0)
    exchange(frames, frame_bits, "frame", t_in, t_into, part, own_frames, 4)

    landed(v_into, 0)
    v_rows = v_got.shape[1] * ROW

    def view_heads(j, _):
        lanes = pl.ds(pl.multiple_of(j * LANES, LANES), LANES)
        block = [v_got[i, :, :, lanes].reshape(v_rows, LANES) for i in range(4)]
        for i, value in enumerate(attention(*block)):
            v_made[i, :, :, lanes] = value.astype(BF16).reshape(v_rows // ROW, ROW, LANES)
        return 0

    lax.fori_loop(0, lane_groups, view_heads, 0)
    exchange(views, view_bits, "view", v_from, v_out, lambda r, i: r.at[i], unit, 8)

    landed(t_into, 4)
    steps = t_got.shape[1]

    def widen(j, _):
        frames_of = pl.ds(j * ROW, ROW)
        rows_of = pl.ds(pl.multiple_of(j * ROW * ROW, ROW * ROW), ROW * ROW)
        for i in range(4):
            rows = t_got[i, frames_of].astype(F32).reshape(ROW * ROW, LANES)
            t_wide[i, 0, rows_of, :] = rows[:, :HALF]
            t_wide[i, 1, rows_of, :] = rows[:, HALF:]
        return 0

    lax.fori_loop(0, steps // ROW, widen, 0)

    def patch(j, _):
        rows_of = pl.ds(j, steps, stride=ROW)
        block = [
            jnp.concatenate([t_wide[i, h, rows_of, :] for h in range(2)], axis=1).astype(BF16)
            for i in range(4)
        ]
        for i, value in enumerate(attention(*block)):
            o_wide[i, 0, rows_of, :] = value[:, :HALF]
            o_wide[i, 1, rows_of, :] = value[:, HALF:]
        return 0

    lax.fori_loop(0, ROW, patch, 0)

    def narrow(j, _):
        frames_of = pl.ds(j * ROW, ROW)
        rows_of = pl.ds(pl.multiple_of(j * ROW * ROW, ROW * ROW), ROW * ROW)
        for i in range(3):
            rows = jnp.concatenate([o_wide[i, h, rows_of, :] for h in range(2)], axis=1)
            t_made[i, frames_of] = rows.astype(BF16).reshape(ROW, ROW, LANES)
        return 0

    lax.fori_loop(0, steps // ROW, narrow, 0)
    exchange(frames, frame_bits, "frame", t_from, t_out, own_frames, part, 11)

    landed(v_out, 8)
    landed(t_out, 11)
    left(views - 1, v_got.at[0], 0, 4)
    left((frames - 1) * local, t_got.at[0], 4, 4)
    left(views - 1, v_made.at[0], 8, 3)
    left((frames - 1) * local, t_made.at[0], 11, 3)


def per_device(frames, views, *arrays):
    shape = arrays[0].shape
    flat = [array.reshape(shape[1:]) for array in arrays]
    whole = frames * shape[1]
    out = pl.pallas_call(
        functools.partial(kernel, frames, views),
        name="both_blocks",
        out_shape=[jax.ShapeDtypeStruct(shape[1:], BF16)] * 6,
        in_specs=[pl.BlockSpec(memory_space=pl.ANY)] * 8,
        out_specs=[pl.BlockSpec(memory_space=pl.ANY)] * 6,
        scratch_shapes=[
            pltpu.VMEM((4, whole, ROW, LANES), BF16),
            pltpu.VMEM((4, views, ROW, shape[3]), BF16),
            pltpu.VMEM((3, whole, ROW, LANES), BF16),
            pltpu.VMEM((3, views, ROW, shape[3]), BF16),
            pltpu.VMEM((4, 2, whole * ROW, HALF), F32),
            pltpu.VMEM((3, 2, whole * ROW, HALF), F32),
            pltpu.SemaphoreType.DMA((14,)),
            pltpu.SemaphoreType.DMA((14,)),
        ],
        compiler_params=pltpu.CompilerParams(collective_id=0, has_side_effects=True),
    )(*flat)
    return tuple(array.reshape(shape) for array in out)


def solution(mesh):
    placed = P("view", "frame", None, None)
    return jax.shard_map(
        functools.partial(per_device, mesh.shape["frame"], mesh.shape["view"]),
        mesh=mesh,
        in_specs=(placed,) * 8,
        out_specs=(placed,) * 6,
        check_vma=False,
    )
```
